32 devices in a mesh: rows: 4 (over y, core), cols: 4 (over z), heads: 2 (over x).
Axes of the slice: x: 2, y: 2, z: 4, core: 2. Of those that a mesh axis runs over, the one named last changes fastest.
Arguments:
- tokens: bfloat16 [16384, 1024], P(('rows', 'cols'), 'heads'), may hold values from -8 to 8
- ln_gain: float32 [1024], replicated, may hold values from 0.1 to 1.9
- w_qkv: bfloat16 [3, 1024, 1024], P(None, None, 'heads'), may hold values from -1 to 1
- w_out: bfloat16 [1024, 1024], P('heads'), may hold values from -0.1875 to 0.1875
- out_bias: float32 [1024], P('heads'), may hold values from -3 to 3
Outputs:
- mixed: bfloat16 [16384, 1024], P(('rows', 'cols'), 'heads')
The draws below stay inside these ranges and needn't reach their ends.
All inputs are finite; a program needn't handle non-finite values.
Results may differ from the reference program's by a relative error of at most 0.0095.
Values may be sent and summed in bfloat16 or wider, within the bound.
A program may use at most 128 MiB of HBM per device.

```python
import jax
import jax.numpy as jnp
from jax import lax

D = 1024
HEADS = 16
TOKENS = 16384
N_HEADS = 2


def draw_tokens(key, part):
    first = jax.random.fold_in(jax.random.fold_in(key, 3), 0)
    base = jax.random.normal(first, (TOKENS, D), jnp.float32)
    return jnp.clip(base, -8.0, 8.0).astype(jnp.bfloat16)


def draw_w_qkv(key, part):
    first = jax.random.fold_in(jax.random.fold_in(key, 5), 0)
    base = jax.random.normal(first, (3, D, D), jnp.float32) * D ** (-0.5)
    spread = jnp.array([1.7, 1.7, 1.0], jnp.float32).reshape(3, 1, 1)
    base = base * spread
    return jnp.clip(base, -1.0, 1.0).astype(jnp.bfloat16)


def block_scale(key, shape, cuts, least, top_value):
    gain, own = 1.0, jax.random.fold_in(key, 6)
    for position, blocks in cuts:
        draws = jnp.exp(jax.random.uniform(jax.random.fold_in(own, position), (blocks,), jnp.float32, least / len(cuts), top_value / len(cuts)))
        gain = gain * jnp.repeat(draws, shape[position] // blocks).reshape([-1 if axis == position else 1 for axis in range(len(shape))])
    return gain


def scatter_about(key, extent, width, reach, cuts=(), held_as=jnp.bfloat16):
    drawn = jax.random.normal(key, extent, jnp.float32) * width
    if len(cuts) > 0:
        drawn = block_scale(key, extent, cuts, -0.22, 0.18) * drawn
    return jnp.clip(drawn, min=-reach, max=reach).astype(held_as)


def setup_inputs(seed: int = 0) -> dict:
    key_of = jax.random.split(jax.random.key(seed), 6)
    tokens = draw_tokens(jax.random.fold_in(key_of[5], 71), 0)
    ln_gain = jnp.clip(1.0 + 0.18 * jax.random.normal(key_of[1], (D,), jnp.float32), 0.1, 1.9)
    w_qkv = draw_w_qkv(jax.random.fold_in(key_of[5], 71), 0)
    w_out = scatter_about(key_of[3], (D, D), D ** -0.5, 0.1875, ((0, 2),))
    out_bias = scatter_about(key_of[4], (D,), 0.5, 3.0, ((0, 2),), jnp.float32)
    return {"tokens": tokens, "ln_gain": ln_gain, "w_qkv": w_qkv, "w_out": w_out, "out_bias": out_bias}


def layer_norm(tokens, ln_gain):
    xf = tokens.astype(jnp.float32)
    mean = lax.optimization_barrier(jnp.mean(xf, axis=-1, keepdims=True))
    centered = xf - mean
    var = lax.optimization_barrier(jnp.mean(centered * centered, axis=-1, keepdims=True))
    return (centered * lax.rsqrt(var + 1e-06) * ln_gain).astype(jnp.bfloat16)

def reference(tokens, ln_gain, w_qkv, w_out, out_bias):
    normed = layer_norm(tokens, ln_gain)
    query = jnp.dot(normed, w_qkv[0], preferred_element_type=jnp.float32).astype(jnp.bfloat16)
    keys = jnp.dot(normed, w_qkv[1], preferred_element_type=jnp.float32).astype(jnp.bfloat16)
    values = jnp.dot(normed, w_qkv[2], preferred_element_type=jnp.float32).astype(jnp.bfloat16)
    head_dim = D // HEADS
    scale = 1.0 / head_dim ** 0.5
    block = 1024 if TOKENS % 1024 == 0 else TOKENS
    nblocks = TOKENS // block
    qt = query.reshape(TOKENS, HEADS, head_dim).transpose(1, 0, 2)
    kt = keys.reshape(TOKENS, HEADS, head_dim).transpose(1, 0, 2)
    vt = values.reshape(TOKENS, HEADS, head_dim).transpose(1, 0, 2)

    def one_head(args):
        qh, kh, vh = args

        def qblock(rows):
            scores = jnp.dot(rows, kh.T, preferred_element_type=jnp.float32) * scale
            peak = lax.optimization_barrier(jnp.max(scores, axis=-1, keepdims=True))
            weights = jnp.exp(scores - peak)
            den = lax.optimization_barrier(jnp.sum(weights, axis=-1, keepdims=True))
            num = jnp.dot(weights.astype(jnp.bfloat16), vh, preferred_element_type=jnp.float32)
            return num / den
        return lax.map(qblock, qh.reshape(nblocks, block, head_dim)).reshape(TOKENS, head_dim)
    attended = lax.map(one_head, (qt, kt, vt))
    attended = attended.transpose(1, 0, 2).reshape(TOKENS, D).astype(jnp.bfloat16)
    group = D // N_HEADS
    summed = jnp.zeros((TOKENS, D), jnp.float32)
    for index in range(N_HEADS):
        part = jnp.dot(attended[:, index * group:(index + 1) * group], w_out[index * group:(index + 1) * group], preferred_element_type=jnp.float32)
        part = lax.optimization_barrier(part.astype(jnp.bfloat16))
        summed = summed + part.astype(jnp.float32)
    return (tokens.astype(jnp.float32) + summed + out_bias).astype(jnp.bfloat16)
```

```python
import functools
import math

import jax
import jax.numpy as jnp
from jax import lax
from jax.experimental import pallas as pl
from jax.experimental.pallas import tpu as pltpu
from jax.sharding import PartitionSpec as P

D = 1024
HEADS = 16
HEAD_DIM = D // HEADS
PAIR = 2 * HEAD_DIM
EXTRA = 16
QB = 256
SAFE = 100.0


def attend_kernel(first, last, info_ref, q_ref, k_ref, v_ref, *rest):
    if not first:
        acc_in, peak_in = rest[:2]
        rest = rest[2:]
    if last:
        out_ref, acc_ref, peak_ref = rest
    else:
        acc_ref, peak_ref = rest
    step = pl.program_id(1)
    heads = q_ref.shape[0]
    rows = v_ref.shape[1] // heads
    kb = k_ref.shape[1]
    qn = q_ref.shape[2]
    qb = min(QB, qn)

    @pl.when(step == 0)
    def _():
        if first:
            acc_ref[...] = jnp.zeros_like(acc_ref)
            peak_ref[...] = jnp.full_like(peak_ref, -jnp.inf)
        else:
            acc_ref[...] = acc_in[...]
            peak_ref[...] = peak_in[...]

    def scores(h, j):
        return jnp.dot(
            k_ref[0], q_ref[h, :, j * qb : (j + 1) * qb], preferred_element_type=jnp.float32
        )

    def weigh(h, probs):
        ones = jnp.ones((EXTRA, kb), jnp.bfloat16)
        lhs = jnp.concatenate([v_ref[0, h * rows : (h + 1) * rows, :], ones], axis=0)
        return jnp.dot(lhs, probs, preferred_element_type=jnp.float32)

    units = [(h, j) for h in range(heads) for j in range(qn // qb)]

    @pl.when(info_ref[1] == 1)
    def _():
        def body(j, carry):
            cols = pl.ds(pl.multiple_of(j * qb, qb), qb)
            all_s = [
                jnp.dot(k_ref[0], q_ref[h, :, cols], preferred_element_type=jnp.float32)
                for h in range(heads)
            ]
            for h in range(heads):
                acc_ref[h, :, cols] += weigh(h, jnp.exp2(all_s[h]).astype(jnp.bfloat16))
            return carry

        lax.fori_loop(0, qn // qb, body, 0, unroll=2)

    @pl.when(info_ref[1] != 1)
    def _():
        for h in range(heads):

            def body(j, carry):
                cols = pl.ds(pl.multiple_of(j * qb, qb), qb)
                s = jnp.dot(k_ref[0], q_ref[h, :, cols], preferred_element_type=jnp.float32)
                old = jnp.max(peak_ref[h, :, cols], axis=0, keepdims=True)
                new = jnp.maximum(old, jnp.max(s, axis=0, keepdims=True))
                probs = jnp.exp2(s - new).astype(jnp.bfloat16)
                acc_ref[h, :, cols] = acc_ref[h, :, cols] * jnp.exp2(old - new) + weigh(h, probs)
                peak_ref[h, :, cols] = jnp.broadcast_to(new, (8, qb))
                return carry

            lax.fori_loop(0, qn // qb, body, 0)

    if last:

        @pl.when(step == pl.num_programs(1) - 1)
        def _():
            for h in range(heads):
                den = jnp.max(acc_ref[h, rows:, :], axis=0, keepdims=True)
                out_ref[h * rows : (h + 1) * rows, :] = (acc_ref[h, :rows, :] / den).astype(jnp.bfloat16)


def attend(info, queries, keys, values, state, first, last, name):
    heads, width, qn = queries.shape
    groups, kb, lanes = keys.shape
    pairs = lanes // PAIR
    steps = groups if first else groups - 1
    tall = HEAD_DIM + EXTRA

    def tile(p, g, info):
        if first:
            return g
        return lax.rem(info[0] + 1 + g, groups)

    in_specs = [
        pl.BlockSpec((2, width, qn), lambda p, g, info: (p, 0, 0)),
        pl.BlockSpec((1, kb, PAIR), lambda p, g, info: (tile(p, g, info), 0, p)),
        pl.BlockSpec((1, PAIR, kb), lambda p, g, info: (tile(p, g, info), p, 0)),
    ]
    state_specs = [
        pl.BlockSpec((2, tall, qn), lambda p, g, info: (p, 0, 0)),
        pl.BlockSpec((2, 8, qn), lambda p, g, info: (p, 0, 0)),
    ]
    state_shapes = [
        jax.ShapeDtypeStruct((heads, tall, qn), jnp.float32),
        jax.ShapeDtypeStruct((heads, 8, qn), jnp.float32),
    ]
    out_specs, out_shape, scratch = state_specs, state_shapes, []
    if last:
        out_specs = [pl.BlockSpec((PAIR, qn), lambda p, g, info: (p, 0))]
        out_shape = [jax.ShapeDtypeStruct((heads * HEAD_DIM, qn), jnp.bfloat16)]
        scratch = [pltpu.VMEM((2, tall, qn), jnp.float32), pltpu.VMEM((2, 8, qn), jnp.float32)]
    args = [queries, keys, values]
    if not first:
        in_specs = in_specs + state_specs
        args += list(state)
    work = heads * steps * kb * qn
    return pl.pallas_call(
        functools.partial(attend_kernel, first, last),
        grid_spec=pltpu.PrefetchScalarGridSpec(
            num_scalar_prefetch=1,
            grid=(pairs, steps),
            in_specs=in_specs,
            out_specs=out_specs,
            scratch_shapes=scratch,
        ),
        out_shape=out_shape,
        compiler_params=pltpu.CompilerParams(
            dimension_semantics=("arbitrary", "arbitrary"), vmem_limit_bytes=48 * 1024 * 1024
        ),
        cost_estimate=pl.CostEstimate(
            flops=16 * HEAD_DIM * work, bytes_accessed=4 * steps * kb * lanes, transcendentals=work
        ),
        name=name,
    )(info, *args)


def per_device(cuts, tokens, ln_gain, w_qkv, w_out, out_bias):
    whole = lax.all_gather(tokens, "heads", axis=1, tiled=True)
    xf = whole.astype(jnp.float32)
    mean = jnp.mean(xf, axis=-1, keepdims=True)
    centered = xf - mean
    var = jnp.mean(centered * centered, axis=-1, keepdims=True)
    normed = (centered * lax.rsqrt(var + 1e-06) * ln_gain).astype(jnp.bfloat16)

    both = ("rows", "cols")
    tok = tokens.shape[0]
    heads = w_out.shape[0] // HEAD_DIM
    keys = jnp.dot(normed, w_qkv[1], preferred_element_type=jnp.float32).astype(jnp.bfloat16)
    values = lax.dot_general(
        w_qkv[2], normed, (((0,), (1,)), ((), ())), preferred_element_type=jnp.float32
    ).astype(jnp.bfloat16)
    edges = [sum(cuts[:i]) * tok // sum(cuts) for i in range(len(cuts) + 1)]
    gathered = []
    for lo, hi in zip(edges[:-1], edges[1:]):
        kg = lax.all_gather(keys[lo:hi], both, axis=0)
        vg = lax.all_gather(values[:, lo:hi], both, axis=0)
        gathered.append((kg, vg))

    factor = math.log2(math.e) / HEAD_DIM**0.5
    queries = (
        lax.dot_general(
            w_qkv[0], normed, (((0,), (1,)), ((), ())), preferred_element_type=jnp.float32
        )
        * factor
    ).astype(jnp.bfloat16)
    byhead = queries.reshape(heads // 2, 2, 1, HEAD_DIM, tok)
    own = jnp.eye(2, dtype=jnp.bfloat16).reshape(1, 2, 2, 1, 1)
    padded = (byhead * own).reshape(heads, PAIR, tok)

    member = jnp.repeat(jnp.eye(heads, dtype=jnp.bfloat16), HEAD_DIM, axis=0)
    ksquare = jnp.square(keys.astype(jnp.float32)).astype(jnp.bfloat16)
    knorm = jnp.max(jnp.dot(ksquare, member, preferred_element_type=jnp.float32), axis=0)
    knorm = lax.pmax(knorm, both)
    qsquare = jnp.square(queries.astype(jnp.float32)).astype(jnp.bfloat16)
    qnorm = jnp.max(jnp.dot(member.T, qsquare, preferred_element_type=jnp.float32), axis=1)
    safe = jnp.all(knorm * qnorm <= SAFE * SAFE)
    info = jnp.stack([lax.axis_index(both).astype(jnp.int32), safe.astype(jnp.int32)])

    state = attend(info, padded, keys[None], values[None], None, True, False, "attend_own")
    for i, (kg, vg) in enumerate(gathered):
        final = i == len(gathered) - 1
        state = attend(info, padded, kg, vg, state, False, final, f"attend_{i}")
    attended = state[0]
    partial_value = lax.dot_general(
        attended, w_out, (((0,), (0,)), ((), ())), preferred_element_type=jnp.float32
    )
    summed = lax.psum_scatter(
        partial_value.astype(jnp.bfloat16), "heads", scatter_dimension=1, tiled=True
    ).astype(jnp.float32)
    return (tokens.astype(jnp.float32) + summed + out_bias).astype(jnp.bfloat16)


def solution(mesh):
    return jax.shard_map(
        functools.partial(per_device, (1, 1)),
        mesh=mesh,
        in_specs=(
            P(("rows", "cols"), "heads"),
            P(),
            P(None, None, "heads"),
            P("heads", None),
            P("heads"),
        ),
        out_specs=P(("rows", "cols"), "heads"),
        check_vma=False,
    )
```
